32 devices in a mesh: groups: 2 (over y), tm: 4 (over z), section: 4 (over x, core).
Axes of the slice: x: 2, y: 2, z: 4, core: 2. Of those that a mesh axis runs over, the one named last changes fastest.
Arguments:
- states: float32 [16, 1, 4096], P(('groups', 'tm')), parts along dimension 0, may hold values from -6 to 6
- timesteps: int32 [16], P(('groups', 'tm')), parts along dimension 0, may hold values from 0 to 999
- step_sizes: float32 [16], P(('groups', 'tm')), parts along dimension 0, may hold values from 0.05 to 0.2
- labels: int32 [2], P('groups'), parts along dimension 0, may hold values from 0 to 1000
- class_table: bfloat16 [1001, 1152], replicated, may hold values from -6 to 6
- embed_weight: bfloat16 [16, 1152], replicated, may hold values from -1.5 to 1.5
- ada_weight: bfloat16 [4, 1152, 2304], P('section', 'tm'), may hold values from -0.1875 to 0.1875
- up_weight: bfloat16 [4, 1152, 2304], P('section', 'tm'), may hold values from -0.1875 to 0.1875
- down_weight: bfloat16 [4, 2304, 1152], P('section', 'tm'), may hold values from -0.125 to 0.125
- final_weight: bfloat16 [1152, 16], replicated, may hold values from -0.1875 to 0.1875
Outputs:
- new_states: float32 [16, 1, 4096], P(('groups', 'tm'), None, 'section'), parts along dimension 0
- step_err: float32 [16], P(('groups', 'tm')), parts along dimension 0
The draws below stay inside these ranges and needn't reach their ends.
There are 2 independent parts, one for each index of `groups`. The reference program is written for one: setup_inputs(seed, part) draws one part's arguments, and reference() takes and returns one part's arrays. A program takes and returns all parts, laid end to end along the dimension named above; an argument that names none is the same for every part. Nothing has to cross between parts.
All inputs are finite; a program needn't handle non-finite values.
Results may differ from the reference program's by a relative error of at most 0.0065.
Values may be sent and summed in bfloat16 or wider, within the bound.
A program may use at most 128 MiB of HBM per device.

```python
import math
import jax
import jax.numpy as jnp
from jax import lax

D = 1152
PATCHES = 256
PCH = 16
CLASSES = 1001
FF = 2304
BATCH = 1
WINDOW = 8
LAYERS = 4
P_SIZE = 4096


def touch_ends(result, own_key, smallest, largest):
    longest = result.shape.index(max(result.shape))
    spots = []
    for shift in (0, 1):
        where = [jax.random.randint(jax.random.fold_in(own_key, axis), (), 0, length) for axis, length in enumerate(result.shape)]
        where[longest] = (where[longest] + shift) % result.shape[longest]
        spots.append(tuple(where))
    return result.at[spots[0]].set(smallest).at[spots[1]].set(largest)


def block_levels(rng, shape, split, smallest, largest):
    level = 1.0
    for dim, shards_of in split:
        draws = jax.random.uniform(jax.random.fold_in(jax.random.fold_in(rng, 6), dim), (shards_of,), jnp.float32, smallest / len(split), largest / len(split))
        level = level * jnp.repeat(jnp.exp(draws), shape[dim] // shards_of).reshape((-1,) + (1,) * (len(shape) - 1 - dim))
    return level


def noise(key, extent, scale, reach, cuts=(), kind=jnp.bfloat16):
    entries = jax.random.normal(key, extent, jnp.float32) * scale
    if len(cuts) > 0:
        entries = block_levels(key, extent, cuts, -0.22, 0.18) * entries
    return jnp.clip(entries, min=-reach, max=reach).astype(kind)


def setup_inputs(seed: int = 0, part: int = 0) -> dict:
    keys = jax.random.split(jax.random.key(seed), 11)
    part_splits = jax.random.split(jax.random.fold_in(keys[10], part), 11)
    states = noise(part_splits[0], (WINDOW, BATCH, P_SIZE), 1.0, 6.0, ((0, 4),), jnp.float32)
    timesteps = touch_ends(jax.random.randint(part_splits[1], (WINDOW,), 0, 1000), jax.random.fold_in(part_splits[1], 1), 0, 999).astype(jnp.int32)
    step_sizes = jnp.clip(jnp.exp(math.log(0.2) - 1.3862944 * jax.random.uniform(part_splits[2], (WINDOW,), jnp.float32) ** block_levels(part_splits[2], (WINDOW,), ((0, 4),), -0.2, 0.2)), 0.05, 0.2)
    labels = jax.random.randint(part_splits[3], (BATCH,), 0, CLASSES).astype(jnp.int32)
    class_table = noise(keys[4], (CLASSES, D), 1.0, 6.0)
    embed_weight = noise(keys[5], (PCH, D), PCH ** -0.5, 1.5)
    ada_weight = noise(keys[6], (LAYERS, D, 2 * D), D ** -0.5, 0.1875, ((0, 4), (1, 4)))
    up_weight = noise(keys[7], (LAYERS, D, FF), D ** -0.5, 0.1875, ((0, 4), (1, 4)))
    down_weight = noise(keys[8], (LAYERS, FF, D), FF ** -0.5, 0.125, ((0, 4), (1, 4)))
    final_weight = noise(keys[9], (D, PCH), D ** -0.5, 0.1875)
    return dict(states=states, timesteps=timesteps, step_sizes=step_sizes, labels=labels, class_table=class_table, embed_weight=embed_weight, ada_weight=ada_weight, up_weight=up_weight, down_weight=down_weight, final_weight=final_weight)


def condition_rows(timesteps, labels, class_table):
    half_width = D // 2
    frequency = jnp.exp(-math.log(10000.0) * jnp.arange(half_width, dtype=jnp.float32) / half_width)
    phases = timesteps.astype(jnp.float32)[:, None] * frequency[None, :]
    timing = jnp.concatenate([jnp.cos(phases), jnp.sin(phases)], axis=1)
    classes = class_table[labels].astype(jnp.float32)
    return jax.nn.silu(timing[:, None, :] + classes[None, :, :]).astype(jnp.bfloat16)

def normalize(values):
    center = values - lax.optimization_barrier(jnp.mean(values, axis=-1, keepdims=True))
    spread = lax.optimization_barrier(jnp.mean(center * center, axis=-1, keepdims=True))
    return center * jax.lax.rsqrt(spread + 1e-06)

def apply_layer(hidden, scale_mod, gate_mod, up_proj, down_proj):
    normed = (normalize(hidden) * (1.0 + scale_mod[:, None, :])).astype(jnp.bfloat16)
    inner = jax.nn.gelu(jnp.dot(normed.reshape(-1, D), up_proj, preferred_element_type=jnp.float32), approximate=True).astype(jnp.bfloat16)
    branch = jnp.dot(inner, down_proj, preferred_element_type=jnp.float32).reshape(hidden.shape)
    return (hidden + gate_mod[:, None, :] * branch).astype(jnp.bfloat16)

def reference(states, timesteps, step_sizes, labels, class_table, embed_weight, ada_weight, up_weight, down_weight, final_weight):
    row_total = WINDOW * BATCH
    cond_rows = condition_rows(timesteps, labels, class_table).reshape(row_total, D)
    patches = states.reshape(row_total, PATCHES, PCH).astype(jnp.bfloat16)
    hidden = jnp.dot(patches.reshape(-1, PCH), embed_weight, preferred_element_type=jnp.float32).reshape(row_total, PATCHES, D)
    for layer in range(LAYERS):
        modulation = jnp.dot(cond_rows, ada_weight[layer], preferred_element_type=jnp.float32)
        hidden = apply_layer(hidden, modulation[:, :D], modulation[:, D:], up_weight[layer], down_weight[layer]).astype(jnp.float32)
    normed = normalize(hidden).astype(jnp.bfloat16)
    drift_rows = jnp.dot(normed.reshape(-1, D), final_weight, preferred_element_type=jnp.float32).reshape(WINDOW, BATCH, P_SIZE)
    term_rows = step_sizes[:, None, None] * drift_rows
    running = jnp.cumsum(term_rows, axis=0)
    earlier = jnp.concatenate([jnp.zeros((1, BATCH, P_SIZE), jnp.float32), running[:-1]], axis=0)
    new_states = states[0][None] + earlier
    step_err = lax.optimization_barrier(jnp.max(jnp.abs(new_states - states), axis=(1, 2)))
    return (new_states, step_err)
```

```python
import functools
import math

import jax
import jax.numpy as jnp
from jax import lax
from jax.experimental import pallas as pl
from jax.experimental.pallas import tpu as pltpu
from jax.sharding import PartitionSpec as P

MESH = pl.DeviceIdType.MESH
F32 = jnp.float32
BF16 = jnp.bfloat16
CORES = 2
LAG = 2


def round_up(value, to):
    return (value + to - 1) // to * to


def pieces_of(columns, limit):
    tiles = columns // 128
    return max(d for d in range(1, limit + 1) if tiles % d == 0)


def worker_of(z, n):
    return z + (1, 0, 0, -1)[z % 4] if n % 4 == 0 else z


def condition_rows(timesteps, labels, class_table):
    width = class_table.shape[1]
    half_width = width // 2
    frequency = jnp.exp(-math.log(10000.0) * jnp.arange(half_width, dtype=F32) / half_width)
    phases = timesteps.astype(F32)[:, None] * frequency[None, :]
    timing = jnp.concatenate([jnp.cos(phases), jnp.sin(phases)], axis=1)
    classes = class_table[labels].astype(F32)
    return jax.nn.silu(timing[:, None, :] + classes[None, :, :]).astype(BF16)


def pad_blocks(array, axis, count, to):
    size = array.shape[axis] // count
    if size == to:
        return array
    shape = array.shape
    array = array.reshape(shape[:axis] + (count, size) + shape[axis + 1 :])
    pads = [(0, 0)] * array.ndim
    pads[axis + 1] = (0, to - size)
    return jnp.pad(array, pads).reshape(shape[:axis] + (count * to,) + shape[axis + 1 :])


def kernel(
    cfg,
    steps_ref,
    cond_ref,
    tokens_ref,
    own_ref,
    embed_ref,
    final_ref,
    ada_ref,
    up_ref,
    down_ref,
    new_ref,
    err_ref,
    up_full,
    down_full,
    condw,
    part,
    modw,
    first,
    hbuf,
    xbuf,
    ubuf,
    mod,
    tok,
    act,
    leave,
    drift_all,
    drift,
    tot,
    tots,
    errs,
    err_own,
    recv_w,
    send_z,
    send_y,
    local_sem,
    cond_send,
    cond_recv,
    mod_send,
    mod_recv,
    patch_send,
    patch_recv,
    first_send,
    first_recv,
    act_send,
    act_recv,
    dr_send,
    dr_recv,
    tot_send,
    tot_recv,
    err_send,
    err_recv,
    go,
):
    n, groups, sections, width = cfg
    z = lax.axis_index("tm")
    g = lax.axis_index("groups")
    s = lax.axis_index("section")
    steps = own_ref.shape[0]
    patches, channels = tokens_ref.shape[0] // steps, tokens_ref.shape[1]
    wpad = final_ref.shape[0]
    fpad = up_ref.shape[1]

    barrier = pltpu.get_barrier_semaphore()
    for axis, size, me in (("tm", n, z), ("groups", groups, g), ("section", sections, s)):
        for k in range(1, size):
            pl.semaphore_signal(
                barrier, inc=1, device_id={axis: lax.rem(me + k, size)}, device_id_type=MESH
            )
    paired = n % 4 == 0
    owners = 2 if paired else 1
    side = lax.rem(z, 4)
    if paired:
        works = (side == 1) | (side == 2)
        inward = jnp.where(side == 0, z + 1, z - 1)
        outward = jnp.where(side == 1, z - 1, z + 1)

        @pl.when(jnp.logical_not(works) & (s < sections - 1))
        def _():
            pl.semaphore_signal(
                barrier,
                inc=1,
                device_id={"tm": inward, "section": sections - 1},
                device_id_type=MESH,
            )

    else:
        works = z >= 0
    greeters = (n - 1) + (groups - 1) + (sections - 1)
    if paired:
        greeters = greeters + jnp.where(works & (s == sections - 1), sections - 1, 0)
    pl.semaphore_wait(barrier, greeters)

    def remote(src, dst, ssem, rsem, axis, to):
        return pltpu.make_async_remote_copy(
            src_ref=src,
            dst_ref=dst,
            send_sem=ssem,
            recv_sem=rsem,
            device_id={axis: to},
            device_id_type=MESH,
        )

    def cond_copy(k):
        to = lax.rem(z + k, n)
        return remote(
            cond_ref.at[to], condw.at[z], cond_send.at[k - 1], cond_recv.at[k - 1], "tm", to
        )

    for k in range(1, n):
        cond_copy(k).start()

    def first_copy(k):
        return remote(own_ref.at[0], first, first_send.at[k - 1], first_recv, "tm", k)

    @pl.when(z == 0)
    def _():
        for k in range(1, n):
            first_copy(k).start()

    def patch_copy():
        return remote(
            tokens_ref, tok.at[pl.ds(steps * patches, steps * patches)], patch_send, patch_recv, "tm", inward
        )

    if paired:

        @pl.when(jnp.logical_not(works) & (s == 0))
        def _():
            patch_copy().start()

    shard = (up_ref, down_ref)
    full = (up_full, down_full)
    pieces = recv_w.shape[2]
    sets = [range(at, min(at + groups, pieces)) for at in range(0, pieces, groups)]
    blocks = owners * steps
    cut = 2 if sections % 2 == 0 else 1
    units, span = blocks * cut, patches // cut
    early = min(CORES, sections - 1)
    leads = lax.rem(s, CORES) == 0
    margin = 1 if paired else 0
    last = n - 1 - margin

    def owner_of(w, p):
        return (w + p) % groups

    def place(w, origin, p):
        rows, columns = shard[w].shape
        size = columns // pieces
        return full[w].at[
            pl.ds(pl.multiple_of(origin * rows, 16), rows), pl.ds(p * size, size)
        ]

    def own_piece(w, p):
        size = shard[w].shape[1] // pieces
        return shard[w].at[:, pl.ds(p * size, size)]

    def along(w, direction, k, p):
        by = 1 - 2 * direction
        origin = z - by * k
        src = own_piece(w, p) if k == 0 else place(w, origin, p)
        return remote(
            src, place(w, origin, p), send_z.at[w, direction, k, p], recv_w.at[w, origin, p], "tm", z + by
        )

    def across(w, direction, k, p, j):
        origin = z - (1 - 2 * direction) * k
        return remote(
            place(w, origin, p),
            place(w, origin, p),
            send_y.at[w, direction, k, p, j - 1],
            recv_w.at[w, origin, p],
            "groups",
            lax.rem(g + j, groups),
        )

    def arrived(w, origin, p):
        return remote(
            place(w, origin, p), place(w, origin, p), send_z.at[w, 0, 0, p], recv_w.at[w, origin, p], "tm", z
        )

    def has_next(direction):
        return (z < n - 1 - margin) if direction == 0 else (z > margin)

    def has_origin(direction, k):
        if direction == 0:
            return (z >= k) & (z < n - margin)
        return (z < n - k) & (z >= margin)

    def at_end(direction):
        return (z == 0) if direction == 0 else (z == n - 1)

    def beside_end(direction):
        return (z == 1) if direction == 0 else (z == n - 2)

    def own_sends(w, members, act_on):
        for case in range(groups):

            @pl.when(g == case)
            def _(case=case):
                for p in sorted(members, key=lambda p: owner_of(w, p) != case):
                    mine = owner_of(w, p) == case
                    for direction in range(2):
                        if mine or paired:

                            @pl.when(has_next(direction) if mine else at_end(direction))
                            def _(direction=direction, p=p):
                                act_on(along(w, direction, 0, p))

    def start(copy):
        copy.start()

    def wait_send(copy):
        copy.wait_send()

    runs = [(w, members) for w in range(2) for members in sets]
    ahead = min(3, len(runs))

    def send_first():
        for at, (w, members) in enumerate(runs):
            if at < ahead:
                own_sends(w, members, start)

    def relay(w, k, members):
        for case in range(groups):

            @pl.when(g == case)
            def _(case=case):
                for p in members:
                    if owner_of(w, p) == case:
                        for direction in range(2):

                            @pl.when(has_origin(direction, k))
                            def _(direction=direction, p=p):
                                arrived(w, z - (1 - 2 * direction) * k, p).wait_recv()

                                @pl.when(has_next(direction))
                                def _():
                                    along(w, direction, k, p).start()

                                for j in range(1, groups):
                                    if paired and k == 1:

                                        @pl.when(jnp.logical_not(beside_end(direction)))
                                        def _(j=j):
                                            across(w, direction, k, p, j).start()

                                    else:
                                        across(w, direction, k, p, j).start()

    def rest_arrived(w, members):
        for case in range(groups):

            @pl.when(g == case)
            def _(case=case):
                for p in members:
                    if owner_of(w, p) != case:
                        for k in range(1, last + 1):
                            for direction in range(2):

                                @pl.when(has_origin(direction, k))
                                def _(direction=direction, k=k, p=p):
                                    arrived(w, z - (1 - 2 * direction) * k, p).wait_recv()

    def local_copy(w):
        rows = shard[w].shape[0]
        return pltpu.make_async_copy(
            shard[w], full[w].at[pl.ds(pl.multiple_of(z * rows, 16), rows), :], local_sem.at[w]
        )

    ends = at_end(0) | at_end(1) if paired else z < 0
    led = leads & (s < sections - 1)

    @pl.when(leads)
    def _():
        send_first()

    for w in range(2):
        local_copy(w).start()

    condw[z] = cond_ref[z]
    for k in range(1, n):
        cond_copy(k).wait()
    pad = condw.shape[1]
    products = jnp.dot(
        condw[...].reshape(n * pad, condw.shape[2]), ada_ref[...], preferred_element_type=F32
    )
    for owner in range(n):
        part[owner] = products[owner * pad : owner * pad + steps]

    def slot_of(owner):
        return 0 if worker_of(owner, n) == owner else 1

    def mod_copy(owner):
        slot = slot_of(owner)
        return remote(
            part.at[owner],
            modw.at[slot, z],
            mod_send.at[owner],
            mod_recv.at[slot, z],
            "tm",
            worker_of(owner, n),
        )

    def mod_arrived(slot, source):
        return remote(
            modw.at[slot, source], modw.at[slot, source], mod_send.at[0], mod_recv.at[slot, source], "tm", z
        )

    for owner in range(n):

        @pl.when(z != worker_of(owner, n))
        def _(owner=owner):
            mod_copy(owner).start()

        @pl.when(z == worker_of(owner, n))
        def _(owner=owner):
            modw[slot_of(owner), z] = part[owner]

    @pl.when(jnp.logical_not(leads))
    def _():
        pl.semaphore_wait(go, 1)
        send_first()

    @pl.when(ends)
    def _():
        for w, members in runs[ahead:]:
            own_sends(w, members, start)

    def release():
        pl.semaphore_signal(go, inc=1, device_id={"section": s + 1}, device_id_type=MESH)

    block = wpad // n
    real = width // n
    if block != real:
        mask = (lax.broadcasted_iota(jnp.int32, (1, wpad), 1) % block < real).astype(F32)

    def normalize(values):
        center = values - jnp.sum(values, axis=-1, keepdims=True) * (1.0 / width)
        if block != real:
            center = center * mask
        spread = jnp.sum(center * center, axis=-1, keepdims=True) * (1.0 / width)
        return center * lax.rsqrt(spread + 1e-06)

    everything = pl.ds(0, units * span)

    def act_copy(u, at=None, rows=None):
        rows = pl.ds(pl.multiple_of(u * span, span), span) if rows is None else rows
        window = (rows, pl.ds(0, wpad) if at is None else at)
        return remote(leave.at[window], act.at[window], act_send.at[u], act_recv.at[u], "section", s + 1)

    def turn(i):
        return lax.rem(i + (owners - 1) * steps * cut, units)

    def modulations():
        for slot in range(owners):
            total = jnp.zeros(modw.shape[2:], F32)
            for source in range(n):

                @pl.when(z != source)
                def _(slot=slot, source=source):
                    mod_arrived(slot, source).wait_recv()

                total = total + modw[slot, source]
            for step in range(steps):
                mod[slot * steps + step] = total[step : step + 1]

    def scaled(b, values):
        return (normalize(values) * (1.0 + mod[b, :, pl.ds(0, wpad)])).astype(BF16)

    def prepare():
        @pl.when(s == 0)
        def _():
            tok[pl.ds(0, steps * patches)] = tokens_ref[...]
            if paired:
                patch_copy().wait_recv()

        @pl.when(s > 0)
        def _():
            act_copy(0, rows=everything).wait_recv()

        def one(b, carry):
            rows = pl.ds(pl.multiple_of(b * patches, patches), patches)

            @pl.when(s == 0)
            def _():
                hbuf[...] = jnp.dot(tok[rows], embed_ref[...], preferred_element_type=F32)

            @pl.when(s > 0)
            def _():
                hbuf[...] = act[rows].astype(F32)

            xbuf[rows] = scaled(b, hbuf[...])
            return carry

        lax.fori_loop(0, blocks, one, 0)

    def columns_of(w, members):
        size = shard[w].shape[1] // pieces
        return pl.ds(members[0] * size, len(members) * size)

    def gelu(values):
        return jax.nn.gelu(values, approximate=True).astype(BF16)

    def early_up(members):
        at = columns_of(0, members)
        ubuf[:, at] = gelu(jnp.dot(xbuf[...], up_full[:, at], preferred_element_type=F32))

    def early_down(members):
        at = columns_of(1, members)
        branch = jnp.dot(ubuf[...], down_full[:, at], preferred_element_type=F32)

        def combine(before):
            for b in range(blocks):
                rows = pl.ds(b * patches, patches)
                gate = mod[b, :, pl.ds(wpad + at.start, at.size)]
                here = gate * branch[b * patches : (b + 1) * patches]
                leave[rows, at] = (before(rows) + here).astype(BF16)

        @pl.when(s == 0)
        def _():
            combine(lambda rows: jnp.dot(tok[rows], embed_ref[:, at], preferred_element_type=F32))

        @pl.when(s > 0)
        def _():
            combine(lambda rows: act[rows, at].astype(F32))

        @pl.when(s + 1 < early)
        def _():
            act_copy(0, at, everything).start()

        @pl.when(s + 1 == early)
        def _():
            for i in range(units // 2):
                act_copy(turn(i), at).start()

    streams = works & (s < early)
    count = len(sets)
    begin = min(3, 2 * count - 1)
    behind = LAG * (last - 1) + 1
    expands = [max(j + behind, begin + 1 + j // 2) for j in range(count)]
    tasks = [(begin, prepare, None)]
    tasks += [(t, early_up, (0, members)) for t, members in zip(expands, sets)]
    tasks += [
        (max(count + j + behind, expands[-1]), early_down, (1, members)) for j, members in enumerate(sets)
    ]

    def do(task):
        _, work, run = task
        if run is not None:
            rest_arrived(*run)

        @pl.when(streams)
        def _():
            if run is None:
                modulations()
                work()
            else:
                work(run[1])

    for w in range(2):
        local_copy(w).wait()

    @pl.when(led & ends)
    def _():
        for w, members in runs[:-1]:
            own_sends(w, members, wait_send)
        release()

    for t in range(len(runs) + LAG * (last - 1)):
        if t + ahead < len(runs):

            @pl.when(jnp.logical_not(ends))
            def _(t=t):
                own_sends(*runs[t + ahead], start)

        for k in range(1, last + 1):
            if 0 <= t - LAG * (k - 1) < len(runs):
                w, members = runs[t - LAG * (k - 1)]
                relay(w, k, members)
        if t == len(runs) - 1:

            @pl.when(led & jnp.logical_not(ends))
            def _():
                release()

        for task in tasks:
            if task[0] == t:
                do(task)
    for task in tasks:
        if task[0] >= len(runs) + LAG * (last - 1):
            do(task)

    @pl.when(streams & (s + 1 == early))
    def _():
        for i in range(units // 2, units):
            act_copy(turn(i)).start()

    def drift_copy(slot, d):
        to = {"tm": jnp.where(slot == 0, z, outward) if paired else z, "section": d}
        return pltpu.make_async_remote_copy(
            src_ref=drift_all.at[d, pl.ds(slot * steps, steps)],
            dst_ref=drift,
            send_sem=dr_send.at[slot, d],
            recv_sem=dr_recv,
            device_id=to,
            device_id_type=MESH,
        )

    tile = 256 if fpad % 256 == 0 else 128

    @pl.when(works & (s >= early))
    def _():
        modulations()

        def one(i, carry):
            u = turn(i)
            b, part_of = u // cut, lax.rem(u, cut)
            rows = pl.ds(pl.multiple_of(u * span, span), span)
            act_copy(u).wait_recv()
            x = scaled(b, act[rows].astype(F32))
            before = None
            for at in range(0, fpad, tile):
                inner = jnp.dot(x, up_full[:, at : at + tile], preferred_element_type=F32)
                if before is not None:
                    ubuf[rows, at - tile : at] = gelu(before)
                before = inner
            ubuf[rows, fpad - tile : fpad] = gelu(before)
            branch = jnp.dot(ubuf[rows], down_full[...], preferred_element_type=F32)
            result = (act[rows].astype(F32) + mod[b, :, pl.ds(wpad, wpad)] * branch).astype(BF16)

            @pl.when(s < sections - 1)
            def _():
                leave[rows] = result
                act_copy(u).start()

            @pl.when(s == sections - 1)
            def _():
                normed = normalize(result.astype(F32)).astype(BF16)
                fresh = jnp.dot(normed, final_ref[...], preferred_element_type=F32)
                share = sections // cut
                drift_all[pl.ds(part_of * share, share), b] = fresh.reshape(
                    (share,) + drift_all.shape[2:]
                )
                for slot in range(owners):

                    @pl.when(u == ((slot + 1) * steps) * cut - 1)
                    def _(slot=slot):
                        for d in range(sections if slot else sections - 1):
                            drift_copy(slot, d).start()

            return carry

        lax.fori_loop(0, units, one, 0)

    here = works & (s == sections - 1)

    @pl.when(here)
    def _():
        drift[...] = drift_all[sections - 1, pl.ds(0, steps)]

    @pl.when(jnp.logical_not(here))
    def _():
        drift_copy(0, 0).wait_recv()

    running = jnp.zeros(tot.shape, F32)
    for b in range(steps):
        running = running + steps_ref[b] * drift[b]
    tot[...] = running

    def tot_copy(k):
        return remote(tot, tots.at[k - 1], tot_send.at[k - 1], tot_recv.at[k - 1], "tm", z + k)

    for k in range(1, n):

        @pl.when(z < n - k)
        def _(k=k):
            tot_copy(k).start()

    @pl.when(z == 0)
    def _():
        first[...] = own_ref[0]

    @pl.when(z > 0)
    def _():
        first_copy(1).wait_recv()

    tot_start = first[...]
    new_ref[0] = jnp.zeros(tot.shape, F32)
    for k in range(n - 1, 0, -1):

        @pl.when(z >= k)
        def _(k=k):
            tot_copy(k).wait_recv()
            new_ref[0] = new_ref[0] + tots[k - 1]

    base = tot_start + new_ref[0]
    running = jnp.zeros(tot.shape, F32)
    errors = []
    for b in range(steps):
        fresh = base + running
        running = running + steps_ref[b] * drift[b]
        new_ref[b] = fresh
        delta = jnp.max(jnp.abs(fresh - own_ref[b]), axis=0, keepdims=True)
        errors.append(jnp.broadcast_to(jnp.max(delta, axis=1, keepdims=True), (1, 128)))
    for b in range(steps):
        err_own[pl.ds(b, 1), :] = errors[b]
    for b in range(steps, err_own.shape[0]):
        err_own[pl.ds(b, 1), :] = jnp.zeros((1, 128), F32)

    def err_copy(k):
        return remote(
            err_own, errs.at[k - 1], err_send.at[k - 1], err_recv.at[k - 1], "section", lax.rem(s + k, sections)
        )

    for k in range(1, sections):
        err_copy(k).start()
    worst = err_own[...]
    for k in range(1, sections):
        err_copy(k).wait()
        worst = jnp.maximum(worst, errs[k - 1])
    err_ref[...] = worst

    @pl.when(z == 0)
    def _():
        for k in range(1, n):
            first_copy(k).wait_send()

    @pl.when(jnp.logical_not(led & ends))
    def _():
        for w, members in runs[:-1]:
            own_sends(w, members, wait_send)

    for w, members in runs[-1:]:
        own_sends(w, members, wait_send)
    for w in range(2):
        for k in range(1, last + 1):
            for case in range(groups):

                @pl.when(g == case)
                def _(w=w, k=k, case=case):
                    for p in range(pieces):
                        if owner_of(w, p) == case:
                            for direction in range(2):

                                @pl.when(has_origin(direction, k))
                                def _(direction=direction, p=p):
                                    @pl.when(has_next(direction))
                                    def _():
                                        along(w, direction, k, p).wait_send()

                                    for j in range(1, groups):
                                        if paired and k == 1:

                                            @pl.when(jnp.logical_not(beside_end(direction)))
                                            def _(j=j):
                                                across(w, direction, k, p, j).wait_send()

                                        else:
                                            across(w, direction, k, p, j).wait_send()

    for owner in range(n):

        @pl.when(z != worker_of(owner, n))
        def _(owner=owner):
            mod_copy(owner).wait_send()

    if paired:

        @pl.when(jnp.logical_not(works) & (s == 0))
        def _():
            patch_copy().wait_send()

    @pl.when(works & (s < sections - 1))
    def _():
        @pl.when(s + 1 < early)
        def _():
            act_copy(0, rows=everything).wait_send()

        @pl.when(s + 1 >= early)
        def _():
            for u in range(units):
                act_copy(u).wait_send()

    @pl.when(here)
    def _():
        for slot in range(owners):
            for d in range(sections if slot else sections - 1):
                drift_copy(slot, d).wait_send()

    for k in range(1, n):

        @pl.when(z < n - k)
        def _(k=k):
            tot_copy(k).wait_send()


def shards(
    sizes,
    states,
    timesteps,
    step_sizes,
    labels,
    class_table,
    embed_weight,
    ada_weight,
    up_weight,
    down_weight,
    final_weight,
):
    n, groups, sections = sizes
    steps, batch, p_size = states.shape
    channels, width = embed_weight.shape
    wide = up_weight.shape[2]
    patches = p_size // channels
    own_patches = patches // sections
    block = round_up(width // n, 16)
    wide_block = round_up(wide // n, 16)
    wpad, fpad = n * block, n * wide_block
    pad = 16
    owners = 2 if n % 4 == 0 else 1
    blocks = owners * steps
    units = blocks * (2 if sections % 2 == 0 else 1)

    cond = condition_rows(timesteps, labels, class_table).reshape(steps, n, width // n)
    cond = jnp.pad(cond.transpose(1, 0, 2), ((0, 0), (0, pad - steps), (0, 0)))
    tokens = states.reshape(steps, patches, channels)
    own = lax.dynamic_slice_in_dim(tokens, lax.axis_index("section") * own_patches, own_patches, 1)
    embed = pad_blocks(embed_weight, 1, n, block)
    final = pad_blocks(final_weight, 0, n, block)
    ada = pad_blocks(ada_weight[0], 1, 2 * n, block)
    up = pad_blocks(pad_blocks(up_weight[0], 1, n, wide_block), 0, 1, block)
    down = pad_blocks(pad_blocks(down_weight[0], 1, n, block), 0, 1, wide_block)
    limit = max(1, 36 // n)
    pieces = max(
        d for d in range(1, limit + 1) if (wpad // 128) % d == 0 and (fpad // 128) % d == 0
    )
    vmem = pltpu.VMEM
    dma = pltpu.SemaphoreType.DMA
    part_shape = (steps, own_patches, channels)
    new_states, errors = pl.pallas_call(
        functools.partial(kernel, (n, groups, sections, width)),
        out_shape=(
            jax.ShapeDtypeStruct(part_shape, F32),
            jax.ShapeDtypeStruct((8, 128), F32),
        ),
        in_specs=[pl.BlockSpec(memory_space=pltpu.SMEM)] + [pl.BlockSpec(memory_space=vmem)] * 8,
        out_specs=(pl.BlockSpec(memory_space=vmem), pl.BlockSpec(memory_space=vmem)),
        scratch_shapes=[
            vmem((wpad, fpad), BF16),
            vmem((fpad, wpad), BF16),
            vmem((n, pad, width // n), BF16),
            vmem((n, steps, 2 * wpad), F32),
            vmem((owners, n, steps, 2 * wpad), F32),
            vmem(part_shape[1:], F32),
            vmem((patches, wpad), F32),
            vmem((blocks * patches, wpad), BF16),
            vmem((blocks * patches, fpad), BF16),
            vmem((blocks, 1, 2 * wpad), F32),
            vmem((blocks * patches, channels), BF16),
            vmem((blocks * patches, wpad), BF16),
            vmem((blocks * patches, wpad), BF16),
            vmem((sections, blocks, own_patches, channels), F32),
            vmem(part_shape, F32),
            vmem(part_shape[1:], F32),
            vmem((max(n - 1, 1),) + part_shape[1:], F32),
            vmem((max(sections - 1, 1), 8, 128), F32),
            vmem((8, 128), F32),
            dma((2, n, pieces)),
            dma((2, 2, n, pieces)),
            dma((2, 2, n, pieces, max(groups - 1, 1))),
            dma((2,)),
            dma((n,)),
            dma((n,)),
            dma((n,)),
            dma((owners, n)),
            dma(()),
            dma(()),
            dma((n,)),
            dma(()),
            dma((units,)),
            dma((units,)),
            dma((owners, sections)),
            dma(()),
            dma((n,)),
            dma((n,)),
            dma((sections,)),
            dma((sections,)),
            pltpu.SemaphoreType.REGULAR,
        ],
        compiler_params=pltpu.CompilerParams(
            collective_id=0, has_side_effects=True, vmem_limit_bytes=60 * 1024 * 1024
        ),
    )(step_sizes, cond, tokens.astype(BF16).reshape(steps * patches, channels), own, embed, final, ada, up, down)
    return new_states.reshape(steps, batch, p_size // sections), errors[:steps, 0]


def solution(mesh):
    sizes = (mesh.shape["tm"], mesh.shape["groups"], mesh.shape["section"])
    return jax.shard_map(
        functools.partial(shards, sizes),
        mesh=mesh,
        in_specs=(
            P(("groups", "tm"), None, None),
            P(("groups", "tm")),
            P(("groups", "tm")),
            P("groups"),
            P(),
            P(),
            P("section", "tm", None),
            P("section", "tm", None),
            P("section", "tm", None),
            P(),
        ),
        out_specs=(P(("groups", "tm"), None, "section"), P(("groups", "tm"))),
        check_vma=False,
    )
```

```python
import functools
import math

import jax
import jax.numpy as jnp
from jax import lax
from jax.experimental import pallas as pl
from jax.experimental.pallas import tpu as pltpu
from jax.sharding import PartitionSpec as P

MESH = pl.DeviceIdType.MESH
F32 = jnp.float32
BF16 = jnp.bfloat16
CORES = 2
LAG = 2
BEGIN = 5


def round_up(value, to):
    return (value + to - 1) // to * to


def pieces_of(columns, limit):
    tiles = columns // 128
    return max(d for d in range(1, limit + 1) if tiles % d == 0)


def worker_of(z, n):
    return z + (1, 0, 0, -1)[z % 4] if n % 4 == 0 else z


def condition_rows(timesteps, labels, class_table):
    width = class_table.shape[1]
    half_width = width // 2
    frequency = jnp.exp(-math.log(10000.0) * jnp.arange(half_width, dtype=F32) / half_width)
    phases = timesteps.astype(F32)[:, None] * frequency[None, :]
    timing = jnp.concatenate([jnp.cos(phases), jnp.sin(phases)], axis=1)
    classes = class_table[labels].astype(F32)
    return jax.nn.silu(timing[:, None, :] + classes[None, :, :]).astype(BF16)


def pad_blocks(array, axis, count, to):
    size = array.shape[axis] // count
    if size == to:
        return array
    shape = array.shape
    array = array.reshape(shape[:axis] + (count, size) + shape[axis + 1 :])
    pads = [(0, 0)] * array.ndim
    pads[axis + 1] = (0, to - size)
    return jnp.pad(array, pads).reshape(shape[:axis] + (count * to,) + shape[axis + 1 :])


def kernel(
    cfg,
    steps_ref,
    cond_ref,
    tokens_ref,
    own_ref,
    embed_ref,
    final_ref,
    ada_ref,
    up_ref,
    down_ref,
    new_ref,
    err_ref,
    up_full,
    down_full,
    condw,
    part,
    flat,
    scales,
    scalew,
    basis,
    left,
    lowpart,
    loww,
    lows,
    modw,
    first,
    hbuf,
    xbuf,
    ubuf,
    mod,
    tok,
    act,
    leave,
    drift_all,
    drift,
    tot,
    tots,
    errs,
    err_own,
    recv_w,
    send_z,
    send_y,
    local_sem,
    cond_send,
    cond_recv,
    mod_send,
    mod_recv,
    patch_send,
    patch_recv,
    first_send,
    first_recv,
    act_send,
    act_recv,
    dr_send,
    dr_recv,
    tot_send,
    tot_recv,
    err_send,
    err_recv,
    go,
    scale_send,
    scale_recv,
    low_send,
    low_recv,
):
    n, groups, sections, width = cfg
    z = lax.axis_index("tm")
    g = lax.axis_index("groups")
    s = lax.axis_index("section")
    steps = own_ref.shape[0]
    patches, channels = tokens_ref.shape[0] // steps, tokens_ref.shape[1]
    wpad = final_ref.shape[1]
    fpad = up_ref.shape[1]

    barrier = pltpu.get_barrier_semaphore()
    for axis, size, me in (("tm", n, z), ("groups", groups, g), ("section", sections, s)):
        for k in range(1, size):
            pl.semaphore_signal(
                barrier, inc=1, device_id={axis: lax.rem(me + k, size)}, device_id_type=MESH
            )
    paired = n % 4 == 0
    owners = 2 if paired else 1
    side = lax.rem(z, 4)
    if paired:
        works = (side == 1) | (side == 2)
        inward = jnp.where(side == 0, z + 1, z - 1)
        outward = jnp.where(side == 1, z - 1, z + 1)

        @pl.when(jnp.logical_not(works) & (s < sections - 1))
        def _():
            pl.semaphore_signal(
                barrier,
                inc=1,
                device_id={"tm": inward, "section": sections - 1},
                device_id_type=MESH,
            )

    else:
        works = z >= 0
    greeters = (n - 1) + (groups - 1) + (sections - 1)
    if paired:
        greeters = greeters + jnp.where(works & (s == sections - 1), sections - 1, 0)
    pl.semaphore_wait(barrier, greeters)

    def remote(src, dst, ssem, rsem, axis, to):
        return pltpu.make_async_remote_copy(
            src_ref=src,
            dst_ref=dst,
            send_sem=ssem,
            recv_sem=rsem,
            device_id={axis: to},
            device_id_type=MESH,
        )

    def cond_copy(k):
        to = lax.rem(z + k, n)
        return remote(
            cond_ref.at[to], condw.at[z], cond_send.at[k - 1], cond_recv.at[k - 1], "tm", to
        )

    for k in range(1, n):
        cond_copy(k).start()

    def first_copy(k):
        return remote(own_ref.at[0], first, first_send.at[k - 1], first_recv, "tm", k)

    @pl.when(z == 0)
    def _():
        for k in range(1, n):
            first_copy(k).start()

    def patch_copy():
        return remote(
            tokens_ref, tok.at[pl.ds(steps * patches, steps * patches)], patch_send, patch_recv, "tm", inward
        )

    if paired:

        @pl.when(jnp.logical_not(works) & (s == 0))
        def _():
            patch_copy().start()

    shard = (up_ref, down_ref)
    full = (up_full, down_full)
    pieces = recv_w.shape[2]
    sets = [range(at, min(at + groups, pieces)) for at in range(0, pieces, groups)]
    blocks = owners * steps
    cut = 2 if sections % 2 == 0 else 1
    units, span = blocks * cut, patches // cut
    early = min(CORES, sections - 1)
    leads = lax.rem(s, CORES) == 0
    margin = 1 if paired else 0
    last = n - 1 - margin

    def owner_of(w, p):
        return (w + p) % groups

    def place(w, origin, p):
        rows, columns = shard[w].shape
        size = columns // pieces
        return full[w].at[
            pl.ds(pl.multiple_of(origin * rows, 16), rows), pl.ds(p * size, size)
        ]

    def own_piece(w, p):
        size = shard[w].shape[1] // pieces
        return shard[w].at[:, pl.ds(p * size, size)]

    def along(w, direction, k, p):
        by = 1 - 2 * direction
        origin = z - by * k
        src = own_piece(w, p) if k == 0 else place(w, origin, p)
        return remote(
            src, place(w, origin, p), send_z.at[w, direction, k, p], recv_w.at[w, origin, p], "tm", z + by
        )

    def across(w, direction, k, p, j):
        origin = z - (1 - 2 * direction) * k
        return remote(
            place(w, origin, p),
            place(w, origin, p),
            send_y.at[w, direction, k, p, j - 1],
            recv_w.at[w, origin, p],
            "groups",
            lax.rem(g + j, groups),
        )

    def arrived(w, origin, p):
        return remote(
            place(w, origin, p), place(w, origin, p), send_z.at[w, 0, 0, p], recv_w.at[w, origin, p], "tm", z
        )

    def has_next(direction):
        return (z < n - 1 - margin) if direction == 0 else (z > margin)

    def has_origin(direction, k):
        if direction == 0:
            return (z >= k) & (z < n - margin)
        return (z < n - k) & (z >= margin)

    def at_end(direction):
        return (z == 0) if direction == 0 else (z == n - 1)

    def beside_end(direction):
        return (z == 1) if direction == 0 else (z == n - 2)

    def own_sends(w, members, act_on):
        for case in range(groups):

            @pl.when(g == case)
            def _(case=case):
                for p in sorted(members, key=lambda p: owner_of(w, p) != case):
                    mine = owner_of(w, p) == case
                    for direction in range(2):
                        if mine or paired:

                            @pl.when(has_next(direction) if mine else at_end(direction))
                            def _(direction=direction, p=p):
                                act_on(along(w, direction, 0, p))

    def start(copy):
        copy.start()

    def wait_send(copy):
        copy.wait_send()

    runs = [(w, members) for w in range(2) for members in sets]
    ahead = min(3, len(runs))
    opening, early_waits = min(2, len(sets)), len(sets) - 1

    count = len(sets)

    def needs(at, act_on):
        if at < count:
            pl.when(s > 0)(act_on)
        else:
            act_on()

    def send_first():
        @pl.when(s > 0)
        def _():
            for run in runs[:ahead]:
                own_sends(*run, start)

        @pl.when(s == 0)
        def _():
            own_sends(*runs[count], start)

    def waits_early(at):
        def act_on():
            own_sends(*runs[at], wait_send)

        pl.when((s > 0) if not count <= at < count + early_waits else s >= 0)(act_on)

    def send_later(at):
        if at < count + opening:

            @pl.when(s > 0)
            def _():
                own_sends(*runs[at], start)

        else:
            own_sends(*runs[at], start)

    def relay(w, k, members):
        for case in range(groups):

            @pl.when(g == case)
            def _(case=case):
                for p in members:
                    if owner_of(w, p) == case:
                        for direction in range(2):

                            @pl.when(has_origin(direction, k))
                            def _(direction=direction, p=p):
                                arrived(w, z - (1 - 2 * direction) * k, p).wait_recv()

                                @pl.when(has_next(direction))
                                def _():
                                    along(w, direction, k, p).start()

                                for j in range(1, groups):
                                    if paired and k == 1:

                                        @pl.when(jnp.logical_not(beside_end(direction)))
                                        def _(j=j):
                                            across(w, direction, k, p, j).start()

                                    else:
                                        across(w, direction, k, p, j).start()

    def rest_arrived(w, members):
        for case in range(groups):

            @pl.when(g == case)
            def _(case=case):
                for p in members:
                    if owner_of(w, p) != case:
                        for k in range(1, last + 1):
                            for direction in range(2):

                                @pl.when(has_origin(direction, k))
                                def _(direction=direction, k=k, p=p):
                                    arrived(w, z - (1 - 2 * direction) * k, p).wait_recv()

    def local_copy(w):
        rows = shard[w].shape[0]
        return pltpu.make_async_copy(
            shard[w], full[w].at[pl.ds(pl.multiple_of(z * rows, 16), rows), :], local_sem.at[w]
        )

    ends = at_end(0) | at_end(1) if paired else z < 0
    led = leads & (s < sections - 1)

    @pl.when(leads)
    def _():
        send_first()

    for w in range(2):
        local_copy(w).start()

    condw[z] = cond_ref[z]
    for k in range(1, n):
        cond_copy(k).wait()
    pad = condw.shape[1]
    products = jnp.dot(
        condw[...].reshape(n * pad, condw.shape[2]), ada_ref[...], preferred_element_type=F32
    )
    for owner in range(n):
        part[owner] = products[owner * pad : owner * pad + steps]
        flat[pl.ds(owner * steps, steps)] = products[owner * pad : owner * pad + steps, :wpad]
    block = wpad // n
    real = width // n

    def scale_copy(k):
        to = lax.rem(z + k, n)
        return remote(
            scales.at[to], scalew.at[z], scale_send.at[k - 1], scale_recv.at[k - 1], "tm", to
        )

    @pl.when(s == 0)
    def _():
        for owner in range(n):
            scales[owner] = flat[:, owner * block : (owner + 1) * block]
        for k in range(1, n):
            scale_copy(k).start()
        for run in runs[count + 1 : count + opening]:
            own_sends(*run, start)
        scalew[z] = scales[z]

    def slot_of(owner):
        return 0 if worker_of(owner, n) == owner else 1

    def mod_copy(owner):
        slot = slot_of(owner)
        return remote(
            part.at[owner],
            modw.at[slot, z],
            mod_send.at[owner],
            mod_recv.at[slot, z],
            "tm",
            worker_of(owner, n),
        )

    def mod_arrived(slot, source):
        return remote(
            modw.at[slot, source], modw.at[slot, source], mod_send.at[0], mod_recv.at[slot, source], "tm", z
        )

    for owner in range(n):

        @pl.when(z != worker_of(owner, n))
        def _(owner=owner):
            mod_copy(owner).start()

        @pl.when(z == worker_of(owner, n))
        def _(owner=owner):
            modw[slot_of(owner), z] = part[owner]

    def low_copy(owner):
        slot = slot_of(owner)
        return remote(
            lowpart.at[owner],
            loww.at[slot, z],
            low_send.at[owner],
            low_recv.at[slot, z],
            "tm",
            worker_of(owner, n),
        )

    def low_arrived(slot, source):
        return remote(
            loww.at[slot, source], loww.at[slot, source], low_send.at[0], low_recv.at[slot, source], "tm", z
        )

    @pl.when(s == 0)
    def _():
        embed = embed_ref[...].astype(F32)
        embed = embed - jnp.sum(embed, axis=-1, keepdims=True) * (1.0 / width)
        for owner in range(n):

            @pl.when(z == owner)
            def _(owner=owner):
                basis[...] = embed[:, owner * block : (owner + 1) * block]

        for k in range(1, n):
            scale_copy(k).wait()
        total = scalew[0]
        for source in range(1, n):
            total = total + scalew[source]
        for row in range(n * steps):
            left[pl.ds(row * channels, channels)] = (
                basis[...] * (1.0 + total[row : row + 1])
            ).astype(BF16)
        group_rows = steps * channels
        low = jnp.dot(left[...], up_ref[...], preferred_element_type=F32).astype(BF16)
        for owner in range(n):
            lowpart[owner] = low[owner * group_rows : (owner + 1) * group_rows]
        for owner in range(n):

            @pl.when(z != worker_of(owner, n))
            def _(owner=owner):
                low_copy(owner).start()

            @pl.when(z == worker_of(owner, n))
            def _(owner=owner):
                loww[slot_of(owner), z] = lowpart[owner]

    @pl.when(jnp.logical_not(leads))
    def _():
        pl.semaphore_wait(go, 1)
        send_first()

    @pl.when(ends)
    def _():
        for at in range(ahead, len(runs)):
            send_later(at)

    def release():
        pl.semaphore_signal(go, inc=1, device_id={"section": s + 1}, device_id_type=MESH)

    if block != real:
        mask = (lax.broadcasted_iota(jnp.int32, (1, wpad), 1) % block < real).astype(F32)

    def centered(values):
        center = values - jnp.sum(values, axis=-1, keepdims=True) * (1.0 / width)
        return center * mask if block != real else center

    def inverse_spread(center):
        spread = jnp.sum(center * center, axis=-1, keepdims=True) * (1.0 / width)
        return lax.rsqrt(spread + 1e-06)

    def normalize(values):
        center = centered(values)
        return center * inverse_spread(center)

    tile = 256 if fpad % 256 == 0 else 128
    everything = pl.ds(0, units * span)

    def act_copy(u, at=None, rows=None):
        rows = pl.ds(pl.multiple_of(u * span, span), span) if rows is None else rows
        window = (rows, pl.ds(0, wpad) if at is None else at)
        return remote(leave.at[window], act.at[window], act_send.at[u], act_recv.at[u], "section", s + 1)

    def turn(i):
        return lax.rem(i + (owners - 1) * steps * cut, units)

    def modulations():
        for slot in range(owners):
            total = jnp.zeros(modw.shape[2:], F32)
            for source in range(n):

                @pl.when(z != source)
                def _(slot=slot, source=source):
                    mod_arrived(slot, source).wait_recv()

                total = total + modw[slot, source]
            for step in range(steps):
                mod[slot * steps + step] = total[step : step + 1]

    def scaled(b, values):
        return (normalize(values) * (1.0 + mod[b, :, pl.ds(0, wpad)])).astype(BF16)

    def prepare():
        act_copy(0, rows=everything).wait_recv()

        def one(b, carry):
            rows = pl.ds(pl.multiple_of(b * patches, patches), patches)
            xbuf[rows] = scaled(b, act[rows].astype(F32))
            return carry

        lax.fori_loop(0, blocks, one, 0)

    def prepare_first():
        tok[pl.ds(0, steps * patches)] = tokens_ref[...]
        if paired:
            patch_copy().wait_recv()
        for slot in range(owners):
            total = jnp.zeros(loww.shape[2:], F32)
            for source in range(n):

                @pl.when(z != source)
                def _(slot=slot, source=source):
                    low_arrived(slot, source).wait_recv()

                total = total + loww[slot, source].astype(F32)
            total = total.astype(BF16)
            for step in range(steps):
                lows[slot * steps + step] = total[step * channels : (step + 1) * channels]

    def expand_first(b):
        rows = pl.ds(b * patches, patches)
        values = jnp.dot(tok[rows], embed_ref[...], preferred_element_type=F32)
        inverse = inverse_spread(centered(values))
        for at in range(0, fpad, tile):
            inner = jnp.dot(tok[rows], lows[b, :, at : at + tile], preferred_element_type=F32)
            ubuf[rows, at : at + tile] = gelu(inner * inverse)

    def columns_of(w, members):
        size = shard[w].shape[1] // pieces
        return pl.ds(members[0] * size, len(members) * size)

    def gelu(values):
        return jax.nn.gelu(values, approximate=True).astype(BF16)

    def early_up(members):
        at = columns_of(0, members)
        ubuf[:, at] = gelu(jnp.dot(xbuf[...], up_full[:, at], preferred_element_type=F32))

    def early_down(members):
        at = columns_of(1, members)
        branch = jnp.dot(ubuf[...], down_full[:, at], preferred_element_type=F32)

        def combine(before):
            for b in range(blocks):
                rows = pl.ds(b * patches, patches)
                gate = mod[b, :, pl.ds(wpad + at.start, at.size)]
                here = gate * branch[b * patches : (b + 1) * patches]
                leave[rows, at] = (before(rows) + here).astype(BF16)

        @pl.when(s == 0)
        def _():
            combine(lambda rows: jnp.dot(tok[rows], embed_ref[:, at], preferred_element_type=F32))

        @pl.when(s > 0)
        def _():
            combine(lambda rows: act[rows, at].astype(F32))

        @pl.when(s + 1 < early)
        def _():
            act_copy(0, at, everything).start()

        @pl.when(s + 1 == early)
        def _():
            for i in range(units // 2):
                act_copy(turn(i), at).start()

    streams = works & (s < early)
    begin = min(BEGIN, 2 * count - 1)
    behind = LAG * (last - 1) + 1
    expands = [max(j + behind, begin + 1 + j // 2) for j in range(count)]
    finish = len(runs) + LAG * (last - 1)
    one, rest = streams & (s == 0), streams & (s > 0)
    tasks = [(count + behind, one, prepare_first, None, ())]
    tasks += [(count + behind + b, one, expand_first, None, (b,)) for b in range(blocks)]
    tasks += [(finish, one, early_down, (1, members), (members,)) for members in sets]
    tasks += [(begin, rest, prepare, None, ())]
    tasks += [(t, rest, early_up, (0, members), (members,)) for t, members in zip(expands, sets)]
    tasks += [
        (max(count + j + behind, expands[-1]), rest, early_down, (1, members), (members,))
        for j, members in enumerate(sets)
    ]
    def settle(run, where):
        pl.when(where)(lambda: rest_arrived(*run))

    def do(task):
        _, where, work, run, given = task
        if run is not None:
            settle(run, (s == 0) if where is one else (s > 0))

        @pl.when(where)
        def _():
            if work in (prepare, prepare_first):
                modulations()
            work(*given)

    for w in range(2):
        local_copy(w).wait()

    @pl.when(led & ends)
    def _():
        for at in range(len(runs) - 1):
            waits_early(at)
        release()

    for t in range(finish):
        if t + ahead < len(runs):

            @pl.when(jnp.logical_not(ends))
            def _(t=t):
                send_later(t + ahead)

        for k in range(1, last + 1):
            if 0 <= t - LAG * (k - 1) < len(runs):
                at = t - LAG * (k - 1)
                needs(at, lambda at=at, k=k: relay(runs[at][0], k, runs[at][1]))
        if t == len(runs) - 1:

            @pl.when(led & jnp.logical_not(ends))
            def _():
                release()

        for task in tasks:
            if task[0] == t:
                do(task)
    for task in tasks:
        if task[0] >= finish:
            do(task)

    @pl.when(streams & (s + 1 == early))
    def _():
        for i in range(units // 2, units):
            act_copy(turn(i)).start()

    def drift_copy(slot, d):
        to = {"tm": jnp.where(slot == 0, z, outward) if paired else z, "section": d}
        return pltpu.make_async_remote_copy(
            src_ref=drift_all.at[d, pl.ds(slot * steps, steps)],
            dst_ref=drift,
            send_sem=dr_send.at[slot, d],
            recv_sem=dr_recv,
            device_id=to,
            device_id_type=MESH,
        )

    def project(u):
        rows = pl.ds(pl.multiple_of(u * span, span), span)
        normed = normalize(leave[rows].astype(F32)).astype(BF16)
        fresh = lax.dot_general(
            normed, final_ref[...], (((1,), (1,)), ((), ())), preferred_element_type=F32
        )
        share = sections // cut
        drift_all[pl.ds(lax.rem(u, cut) * share, share), u // cut] = fresh.reshape(
            (share,) + drift_all.shape[2:]
        )

    @pl.when(works & (s >= early))
    def _():
        modulations()

        def one(i, carry):
            u = turn(i)
            b = u // cut
            rows = pl.ds(pl.multiple_of(u * span, span), span)
            act_copy(u).wait_recv()
            x = scaled(b, act[rows].astype(F32))
            before = None
            for at in range(0, fpad, tile):
                inner = jnp.dot(x, up_full[:, at : at + tile], preferred_element_type=F32)
                if before is not None:
                    ubuf[rows, at - tile : at] = gelu(before)
                before = inner
            ubuf[rows, fpad - tile : fpad] = gelu(before)
            branch = jnp.dot(ubuf[rows], down_full[...], preferred_element_type=F32)
            result = (act[rows].astype(F32) + mod[b, :, pl.ds(wpad, wpad)] * branch).astype(BF16)

            project(turn(jnp.maximum(i - 1, 0)))
            leave[rows] = result

            @pl.when(s < sections - 1)
            def _():
                act_copy(u).start()

            if owners > 1:

                @pl.when((s == sections - 1) & (i == steps * cut))
                def _():
                    for d in range(sections):
                        drift_copy(1, d).start()

            return carry

        first_rows = pl.ds(turn(0) * span, span)
        leave[first_rows] = jnp.zeros((span, wpad), BF16)
        lax.fori_loop(0, units, one, 0)

        @pl.when(s == sections - 1)
        def _():
            project(turn(units - 1))
            for d in range(sections - 1):
                drift_copy(0, d).start()

    here = works & (s == sections - 1)

    @pl.when(here)
    def _():
        drift[...] = drift_all[sections - 1, pl.ds(0, steps)]

    @pl.when(jnp.logical_not(here))
    def _():
        drift_copy(0, 0).wait_recv()

    running = jnp.zeros(tot.shape, F32)
    for b in range(steps):
        running = running + steps_ref[b] * drift[b]
    tot[...] = running

    def tot_copy(k):
        return remote(tot, tots.at[k - 1], tot_send.at[k - 1], tot_recv.at[k - 1], "tm", z + k)

    for k in range(1, n):

        @pl.when(z < n - k)
        def _(k=k):
            tot_copy(k).start()

    @pl.when(z == 0)
    def _():
        first[...] = own_ref[0]

    @pl.when(z > 0)
    def _():
        first_copy(1).wait_recv()

    tot_start = first[...]
    new_ref[0] = jnp.zeros(tot.shape, F32)
    for k in range(n - 1, 0, -1):

        @pl.when(z >= k)
        def _(k=k):
            tot_copy(k).wait_recv()
            new_ref[0] = new_ref[0] + tots[k - 1]

    base = tot_start + new_ref[0]
    running = jnp.zeros(tot.shape, F32)
    errors = []
    for b in range(steps):
        fresh = base + running
        running = running + steps_ref[b] * drift[b]
        new_ref[b] = fresh
        delta = jnp.max(jnp.abs(fresh - own_ref[b]), axis=0, keepdims=True)
        errors.append(jnp.broadcast_to(jnp.max(delta, axis=1, keepdims=True), (1, 128)))
    for b in range(steps):
        err_own[pl.ds(b, 1), :] = errors[b]
    for b in range(steps, err_own.shape[0]):
        err_own[pl.ds(b, 1), :] = jnp.zeros((1, 128), F32)

    def err_copy(k):
        return remote(
            err_own, errs.at[k - 1], err_send.at[k - 1], err_recv.at[k - 1], "section", lax.rem(s + k, sections)
        )

    for k in range(1, sections):
        err_copy(k).start()
    worst = err_own[...]
    for k in range(1, sections):
        err_copy(k).wait()
        worst = jnp.maximum(worst, errs[k - 1])
    err_ref[...] = worst

    @pl.when(z == 0)
    def _():
        for k in range(1, n):
            first_copy(k).wait_send()

    @pl.when(jnp.logical_not(led & ends))
    def _():
        for at in range(len(runs) - 1):
            needs(at, lambda at=at: own_sends(*runs[at], wait_send))

    @pl.when(led & ends & (s == 0))
    def _():
        for at in range(count + early_waits, len(runs) - 1):
            own_sends(*runs[at], wait_send)

    own_sends(*runs[-1], wait_send)
    for w in range(2):
        for k in range(1, last + 1):
            for case in range(groups):

                @pl.when((g == case) if w else (g == case) & (s > 0))
                def _(w=w, k=k, case=case):
                    for p in range(pieces):
                        if owner_of(w, p) == case:
                            for direction in range(2):

                                @pl.when(has_origin(direction, k))
                                def _(direction=direction, p=p):
                                    @pl.when(has_next(direction))
                                    def _():
                                        along(w, direction, k, p).wait_send()

                                    for j in range(1, groups):
                                        if paired and k == 1:

                                            @pl.when(jnp.logical_not(beside_end(direction)))
                                            def _(j=j):
                                                across(w, direction, k, p, j).wait_send()

                                        else:
                                            across(w, direction, k, p, j).wait_send()

    for owner in range(n):

        @pl.when(z != worker_of(owner, n))
        def _(owner=owner):
            mod_copy(owner).wait_send()

            @pl.when(s == 0)
            def _():
                low_copy(owner).wait_send()

    if paired:

        @pl.when(jnp.logical_not(works) & (s == 0))
        def _():
            patch_copy().wait_send()

    @pl.when(works & (s < sections - 1))
    def _():
        @pl.when(s + 1 < early)
        def _():
            act_copy(0, rows=everything).wait_send()

        @pl.when(s + 1 >= early)
        def _():
            for u in range(units):
                act_copy(u).wait_send()

    @pl.when(here)
    def _():
        for slot in range(owners):
            for d in range(sections if slot else sections - 1):
                drift_copy(slot, d).wait_send()

    for k in range(1, n):

        @pl.when(z < n - k)
        def _(k=k):
            tot_copy(k).wait_send()


def shards(
    sizes,
    states,
    timesteps,
    step_sizes,
    labels,
    class_table,
    embed_weight,
    ada_weight,
    up_weight,
    down_weight,
    final_weight,
):
    n, groups, sections = sizes
    steps, batch, p_size = states.shape
    channels, width = embed_weight.shape
    wide = up_weight.shape[2]
    patches = p_size // channels
    own_patches = patches // sections
    block = round_up(width // n, 16)
    wide_block = round_up(wide // n, 16)
    wpad, fpad = n * block, n * wide_block
    pad = 16
    owners = 2 if n % 4 == 0 else 1
    blocks = owners * steps
    units = blocks * (2 if sections % 2 == 0 else 1)

    cond = condition_rows(timesteps, labels, class_table).reshape(steps, n, width // n)
    cond = jnp.pad(cond.transpose(1, 0, 2), ((0, 0), (0, pad - steps), (0, 0)))
    tokens = states.reshape(steps, patches, channels)
    own = lax.dynamic_slice_in_dim(tokens, lax.axis_index("section") * own_patches, own_patches, 1)
    embed = pad_blocks(embed_weight, 1, n, block)
    final = pad_blocks(final_weight.T, 1, n, block)
    ada = pad_blocks(ada_weight[0], 1, 2 * n, block)
    up = pad_blocks(pad_blocks(up_weight[0], 1, n, wide_block), 0, 1, block)
    down = pad_blocks(pad_blocks(down_weight[0], 1, n, block), 0, 1, wide_block)
    limit = max(1, 36 // n)
    pieces = max(
        d for d in range(1, limit + 1) if (wpad // 128) % d == 0 and (fpad // 128) % d == 0
    )
    vmem = pltpu.VMEM
    dma = pltpu.SemaphoreType.DMA
    part_shape = (steps, own_patches, channels)
    new_states, errors = pl.pallas_call(
        functools.partial(kernel, (n, groups, sections, width)),
        out_shape=(
            jax.ShapeDtypeStruct(part_shape, F32),
            jax.ShapeDtypeStruct((8, 128), F32),
        ),
        in_specs=[pl.BlockSpec(memory_space=pltpu.SMEM)] + [pl.BlockSpec(memory_space=vmem)] * 8,
        out_specs=(pl.BlockSpec(memory_space=vmem), pl.BlockSpec(memory_space=vmem)),
        scratch_shapes=[
            vmem((wpad, fpad), BF16),
            vmem((fpad, wpad), BF16),
            vmem((n, pad, width // n), BF16),
            vmem((n, steps, 2 * wpad), F32),
            vmem((n * steps, wpad), F32),
            vmem((n, n * steps, block), F32),
            vmem((n, n * steps, block), F32),
            vmem((channels, block), F32),
            vmem((n * steps * channels, block), BF16),
            vmem((n, steps * channels, fpad), BF16),
            vmem((owners, n, steps * channels, fpad), BF16),
            vmem((blocks, channels, fpad), BF16),
            vmem((owners, n, steps, 2 * wpad), F32),
            vmem(part_shape[1:], F32),
            vmem((patches, wpad), F32),
            vmem((blocks * patches, wpad), BF16),
            vmem((blocks * patches, fpad), BF16),
            vmem((blocks, 1, 2 * wpad), F32),
            vmem((blocks * patches, channels), BF16),
            vmem((blocks * patches, wpad), BF16),
            vmem((blocks * patches, wpad), BF16),
            vmem((sections, blocks, own_patches, channels), F32),
            vmem(part_shape, F32),
            vmem(part_shape[1:], F32),
            vmem((max(n - 1, 1),) + part_shape[1:], F32),
            vmem((max(sections - 1, 1), 8, 128), F32),
            vmem((8, 128), F32),
            dma((2, n, pieces)),
            dma((2, 2, n, pieces)),
            dma((2, 2, n, pieces, max(groups - 1, 1))),
            dma((2,)),
            dma((n,)),
            dma((n,)),
            dma((n,)),
            dma((owners, n)),
            dma(()),
            dma(()),
            dma((n,)),
            dma(()),
            dma((units,)),
            dma((units,)),
            dma((owners, sections)),
            dma(()),
            dma((n,)),
            dma((n,)),
            dma((sections,)),
            dma((sections,)),
            pltpu.SemaphoreType.REGULAR,
            dma((n,)),
            dma((n,)),
            dma((n,)),
            dma((owners, n)),
        ],
        compiler_params=pltpu.CompilerParams(
            collective_id=0, has_side_effects=True, vmem_limit_bytes=60 * 1024 * 1024
        ),
    )(step_sizes, cond, tokens.astype(BF16).reshape(steps * patches, channels), own, embed, final, ada, up, down)
    return new_states.reshape(steps, batch, p_size // sections), errors[:steps, 0]


def solution(mesh):
    sizes = (mesh.shape["tm"], mesh.shape["groups"], mesh.shape["section"])
    return jax.shard_map(
        functools.partial(shards, sizes),
        mesh=mesh,
        in_specs=(
            P(("groups", "tm"), None, None),
            P(("groups", "tm")),
            P(("groups", "tm")),
            P("groups"),
            P(),
            P(),
            P("section", "tm", None),
            P("section", "tm", None),
            P("section", "tm", None),
            P(),
        ),
        out_specs=(P(("groups", "tm"), None, "section"), P(("groups", "tm"))),
        check_vma=False,
    )
```

```python
import functools
import math

import jax
import jax.numpy as jnp
from jax import lax
from jax.experimental import pallas as pl
from jax.experimental.pallas import tpu as pltpu
from jax.sharding import PartitionSpec as P

MESH = pl.DeviceIdType.MESH
F32 = jnp.float32
BF16 = jnp.bfloat16
CORES = 2
LAG = 2
BEGIN = 5


def round_up(value, to):
    return (value + to - 1) // to * to


def pieces_of(columns, limit):
    tiles = columns // 128
    return max(d for d in range(1, limit + 1) if tiles % d == 0)


def worker_of(z, n):
    return z + (1, 0, 0, -1)[z % 4] if n % 4 == 0 else z


def condition_rows(timesteps, labels, class_table):
    width = class_table.shape[1]
    half_width = width // 2
    frequency = jnp.exp(-math.log(10000.0) * jnp.arange(half_width, dtype=F32) / half_width)
    phases = timesteps.astype(F32)[:, None] * frequency[None, :]
    timing = jnp.concatenate([jnp.cos(phases), jnp.sin(phases)], axis=1)
    classes = class_table[labels].astype(F32)
    return jax.nn.silu(timing[:, None, :] + classes[None, :, :]).astype(BF16)


def pad_blocks(array, axis, count, to):
    size = array.shape[axis] // count
    if size == to:
        return array
    shape = array.shape
    array = array.reshape(shape[:axis] + (count, size) + shape[axis + 1 :])
    pads = [(0, 0)] * array.ndim
    pads[axis + 1] = (0, to - size)
    return jnp.pad(array, pads).reshape(shape[:axis] + (count * to,) + shape[axis + 1 :])


def kernel(
    cfg,
    steps_ref,
    cond_ref,
    given_ref,
    embed_ref,
    final_ref,
    ada_ref,
    up_ref,
    down_ref,
    out_ref,
    err_ref,
    up_full,
    down_full,
    condw,
    part,
    flat,
    scales,
    scalew,
    basis,
    left,
    lowpart,
    loww,
    lows,
    modw,
    first,
    hbuf,
    xbuf,
    ubuf,
    mod,
    tok,
    act,
    leave,
    drift_all,
    drift,
    tot,
    tots,
    errs,
    err_own,
    recv_w,
    send_z,
    send_y,
    local_sem,
    cond_send,
    cond_recv,
    mod_send,
    mod_recv,
    patch_send,
    patch_recv,
    first_send,
    first_recv,
    act_send,
    act_recv,
    dr_send,
    dr_recv,
    tot_send,
    tot_recv,
    err_send,
    err_recv,
    go,
    scale_send,
    scale_recv,
    low_send,
    low_recv,
    new_ref,
    states_ref,
):
    n, groups, sections, width = cfg
    z = lax.axis_index("tm")
    g = lax.axis_index("groups")
    s = lax.axis_index("section")
    steps, patches, channels = states_ref.shape
    lanes = given_ref.shape[2] // channels
    for b in range(steps):
        for j in range(lanes):
            states_ref[b, pl.ds(j, given_ref.shape[1], stride=lanes), :] = given_ref[
                b, :, j * channels : (j + 1) * channels
            ]
    held = patches // sections
    wpad = final_ref.shape[1]
    fpad = up_ref.shape[1]

    barrier = pltpu.get_barrier_semaphore()
    for axis, size, me in (("tm", n, z), ("groups", groups, g), ("section", sections, s)):
        for k in range(1, size):
            pl.semaphore_signal(
                barrier, inc=1, device_id={axis: lax.rem(me + k, size)}, device_id_type=MESH
            )
    paired = n % 4 == 0
    owners = 2 if paired else 1
    side = lax.rem(z, 4)
    if paired:
        works = (side == 1) | (side == 2)
        inward = jnp.where(side == 0, z + 1, z - 1)
        outward = jnp.where(side == 1, z - 1, z + 1)

        @pl.when(jnp.logical_not(works) & (s < sections - 1))
        def _():
            pl.semaphore_signal(
                barrier,
                inc=1,
                device_id={"tm": inward, "section": sections - 1},
                device_id_type=MESH,
            )

    else:
        works = z >= 0
    greeters = (n - 1) + (groups - 1) + (sections - 1)
    if paired:
        greeters = greeters + jnp.where(works & (s == sections - 1), sections - 1, 0)
    pl.semaphore_wait(barrier, greeters)

    def remote(src, dst, ssem, rsem, axis, to):
        return pltpu.make_async_remote_copy(
            src_ref=src,
            dst_ref=dst,
            send_sem=ssem,
            recv_sem=rsem,
            device_id={axis: to},
            device_id_type=MESH,
        )

    def cond_copy(k):
        to = lax.rem(z + k, n)
        return remote(
            cond_ref.at[to], condw.at[z], cond_send.at[k - 1], cond_recv.at[k - 1], "tm", to
        )

    for k in range(1, n):
        cond_copy(k).start()

    def own(b):
        return states_ref.at[b, pl.ds(pl.multiple_of(s * held, held), held)]

    def first_copy(k):
        return remote(own(0), first, first_send.at[k - 1], first_recv, "tm", k)

    @pl.when(z == 0)
    def _():
        for k in range(1, n):
            first_copy(k).start()

    @pl.when(s == 0)
    def _():
        for b in range(steps):
            tok[pl.ds(b * patches, patches)] = states_ref[b].astype(BF16)

    def patch_copy():
        return remote(
            tok.at[pl.ds(0, steps * patches)],
            tok.at[pl.ds(steps * patches, steps * patches)],
            patch_send,
            patch_recv,
            "tm",
            inward,
        )

    if paired:

        @pl.when(jnp.logical_not(works) & (s == 0))
        def _():
            patch_copy().start()

    shard = (up_ref, down_ref)
    full = (up_full, down_full)
    pieces = recv_w.shape[2]
    sets = [range(at, min(at + groups, pieces)) for at in range(0, pieces, groups)]
    blocks = owners * steps
    cut = 2 if sections % 2 == 0 else 1
    units, span = blocks * cut, patches // cut
    early = min(CORES, sections - 1)
    leads = lax.rem(s, CORES) == 0
    margin = 1 if paired else 0
    last = n - 1 - margin

    def owner_of(w, p):
        return (w + p) % groups

    def place(w, origin, p):
        rows, columns = shard[w].shape
        size = columns // pieces
        return full[w].at[
            pl.ds(pl.multiple_of(origin * rows, 16), rows), pl.ds(p * size, size)
        ]

    def own_piece(w, p):
        size = shard[w].shape[1] // pieces
        return shard[w].at[:, pl.ds(p * size, size)]

    def along(w, direction, k, p):
        by = 1 - 2 * direction
        origin = z - by * k
        src = own_piece(w, p) if k == 0 else place(w, origin, p)
        return remote(
            src, place(w, origin, p), send_z.at[w, direction, k, p], recv_w.at[w, origin, p], "tm", z + by
        )

    def across(w, direction, k, p, j):
        origin = z - (1 - 2 * direction) * k
        return remote(
            place(w, origin, p),
            place(w, origin, p),
            send_y.at[w, direction, k, p, j - 1],
            recv_w.at[w, origin, p],
            "groups",
            lax.rem(g + j, groups),
        )

    def arrived(w, origin, p):
        return remote(
            place(w, origin, p), place(w, origin, p), send_z.at[w, 0, 0, p], recv_w.at[w, origin, p], "tm", z
        )

    def has_next(direction):
        return (z < n - 1 - margin) if direction == 0 else (z > margin)

    def has_origin(direction, k):
        if direction == 0:
            return (z >= k) & (z < n - margin)
        return (z < n - k) & (z >= margin)

    def at_end(direction):
        return (z == 0) if direction == 0 else (z == n - 1)

    def beside_end(direction):
        return (z == 1) if direction == 0 else (z == n - 2)

    def own_sends(w, members, act_on):
        for case in range(groups):

            @pl.when(g == case)
            def _(case=case):
                for p in sorted(members, key=lambda p: owner_of(w, p) != case):
                    mine = owner_of(w, p) == case
                    for direction in range(2):
                        if mine or paired:

                            @pl.when(has_next(direction) if mine else at_end(direction))
                            def _(direction=direction, p=p):
                                act_on(along(w, direction, 0, p))

    def start(copy):
        copy.start()

    def wait_send(copy):
        copy.wait_send()

    runs = [(w, members) for w in range(2) for members in sets]
    ahead = min(3, len(runs))
    opening, early_waits = min(2, len(sets)), len(sets) - 1

    count = len(sets)

    def needs(at, act_on):
        if at < count:
            pl.when(s > 0)(act_on)
        else:
            act_on()

    def send_first():
        @pl.when(s > 0)
        def _():
            for run in runs[:ahead]:
                own_sends(*run, start)

        @pl.when(s == 0)
        def _():
            own_sends(*runs[count], start)

    def waits_early(at):
        def act_on():
            own_sends(*runs[at], wait_send)

        pl.when((s > 0) if not count <= at < count + early_waits else s >= 0)(act_on)

    def send_later(at):
        if at < count + opening:

            @pl.when(s > 0)
            def _():
                own_sends(*runs[at], start)

        else:
            own_sends(*runs[at], start)

    def relay(w, k, members):
        for case in range(groups):

            @pl.when(g == case)
            def _(case=case):
                for p in members:
                    if owner_of(w, p) == case:
                        for direction in range(2):

                            @pl.when(has_origin(direction, k))
                            def _(direction=direction, p=p):
                                arrived(w, z - (1 - 2 * direction) * k, p).wait_recv()

                                @pl.when(has_next(direction))
                                def _():
                                    along(w, direction, k, p).start()

                                for j in range(1, groups):
                                    if paired and k == 1:

                                        @pl.when(jnp.logical_not(beside_end(direction)))
                                        def _(j=j):
                                            across(w, direction, k, p, j).start()

                                    else:
                                        across(w, direction, k, p, j).start()

    def rest_arrived(w, members):
        for case in range(groups):

            @pl.when(g == case)
            def _(case=case):
                for p in members:
                    if owner_of(w, p) != case:
                        for k in range(1, last + 1):
                            for direction in range(2):

                                @pl.when(has_origin(direction, k))
                                def _(direction=direction, k=k, p=p):
                                    arrived(w, z - (1 - 2 * direction) * k, p).wait_recv()

    def local_copy(w):
        rows = shard[w].shape[0]
        return pltpu.make_async_copy(
            shard[w], full[w].at[pl.ds(pl.multiple_of(z * rows, 16), rows), :], local_sem.at[w]
        )

    ends = at_end(0) | at_end(1) if paired else z < 0
    led = leads & (s < sections - 1)

    @pl.when(leads)
    def _():
        send_first()

    for w in range(2):
        local_copy(w).start()

    condw[z] = cond_ref[z]
    for k in range(1, n):
        cond_copy(k).wait()
    pad = condw.shape[1]
    products = jnp.dot(
        condw[...].reshape(n * pad, condw.shape[2]), ada_ref[...], preferred_element_type=F32
    )
    for owner in range(n):
        part[owner] = products[owner * pad : owner * pad + steps]
        flat[pl.ds(owner * steps, steps)] = products[owner * pad : owner * pad + steps, :wpad]
    block = wpad // n
    real = width // n

    def scale_copy(k):
        to = lax.rem(z + k, n)
        return remote(
            scales.at[to], scalew.at[z], scale_send.at[k - 1], scale_recv.at[k - 1], "tm", to
        )

    @pl.when(s == 0)
    def _():
        for owner in range(n):
            scales[owner] = flat[:, owner * block : (owner + 1) * block]
        for k in range(1, n):
            scale_copy(k).start()
        for run in runs[count + 1 : count + opening]:
            own_sends(*run, start)
        scalew[z] = scales[z]

    def slot_of(owner):
        return 0 if worker_of(owner, n) == owner else 1

    def mod_copy(owner):
        slot = slot_of(owner)
        return remote(
            part.at[owner],
            modw.at[slot, z],
            mod_send.at[owner],
            mod_recv.at[slot, z],
            "tm",
            worker_of(owner, n),
        )

    def mod_arrived(slot, source):
        return remote(
            modw.at[slot, source], modw.at[slot, source], mod_send.at[0], mod_recv.at[slot, source], "tm", z
        )

    for owner in range(n):

        @pl.when(z != worker_of(owner, n))
        def _(owner=owner):
            mod_copy(owner).start()

        @pl.when(z == worker_of(owner, n))
        def _(owner=owner):
            modw[slot_of(owner), z] = part[owner]

    def low_copy(owner):
        slot = slot_of(owner)
        return remote(
            lowpart.at[owner],
            loww.at[slot, z],
            low_send.at[owner],
            low_recv.at[slot, z],
            "tm",
            worker_of(owner, n),
        )

    def low_arrived(slot, source):
        return remote(
            loww.at[slot, source], loww.at[slot, source], low_send.at[0], low_recv.at[slot, source], "tm", z
        )

    @pl.when(s == 0)
    def _():
        embed = embed_ref[...].astype(F32)
        embed = embed - jnp.sum(embed, axis=-1, keepdims=True) * (1.0 / width)
        for owner in range(n):

            @pl.when(z == owner)
            def _(owner=owner):
                basis[...] = embed[:, owner * block : (owner + 1) * block]

        for k in range(1, n):
            scale_copy(k).wait()
        total = scalew[0]
        for source in range(1, n):
            total = total + scalew[source]
        for row in range(n * steps):
            left[pl.ds(row * channels, channels)] = (
                basis[...] * (1.0 + total[row : row + 1])
            ).astype(BF16)
        group_rows = steps * channels
        low = jnp.dot(left[...], up_ref[...], preferred_element_type=F32).astype(BF16)
        for owner in range(n):
            lowpart[owner] = low[owner * group_rows : (owner + 1) * group_rows]
        for owner in range(n):

            @pl.when(z != worker_of(owner, n))
            def _(owner=owner):
                low_copy(owner).start()

            @pl.when(z == worker_of(owner, n))
            def _(owner=owner):
                loww[slot_of(owner), z] = lowpart[owner]

    @pl.when(jnp.logical_not(leads))
    def _():
        pl.semaphore_wait(go, 1)
        send_first()

    @pl.when(ends)
    def _():
        for at in range(ahead, len(runs)):
            send_later(at)

    def release():
        pl.semaphore_signal(go, inc=1, device_id={"section": s + 1}, device_id_type=MESH)

    if block != real:
        mask = (lax.broadcasted_iota(jnp.int32, (1, wpad), 1) % block < real).astype(F32)

    def centered(values):
        center = values - jnp.sum(values, axis=-1, keepdims=True) * (1.0 / width)
        return center * mask if block != real else center

    def inverse_spread(center):
        spread = jnp.sum(center * center, axis=-1, keepdims=True) * (1.0 / width)
        return lax.rsqrt(spread + 1e-06)

    def normalize(values):
        center = centered(values)
        return center * inverse_spread(center)

    tile = 256 if fpad % 256 == 0 else 128
    everything = pl.ds(0, units * span)

    def act_copy(u, at=None, rows=None):
        rows = pl.ds(pl.multiple_of(u * span, span), span) if rows is None else rows
        window = (rows, pl.ds(0, wpad) if at is None else at)
        return remote(leave.at[window], act.at[window], act_send.at[u], act_recv.at[u], "section", s + 1)

    def turn(i):
        return lax.rem(i + (owners - 1) * steps * cut, units)

    def modulations():
        for slot in range(owners):
            total = jnp.zeros(modw.shape[2:], F32)
            for source in range(n):

                @pl.when(z != source)
                def _(slot=slot, source=source):
                    mod_arrived(slot, source).wait_recv()

                total = total + modw[slot, source]
            for step in range(steps):
                mod[slot * steps + step] = total[step : step + 1]

    def scaled(b, values):
        return (normalize(values) * (1.0 + mod[b, :, pl.ds(0, wpad)])).astype(BF16)

    def prepare():
        act_copy(0, rows=everything).wait_recv()

        def one(b, carry):
            rows = pl.ds(pl.multiple_of(b * patches, patches), patches)
            xbuf[rows] = scaled(b, act[rows].astype(F32))
            return carry

        lax.fori_loop(0, blocks, one, 0)

    def prepare_first():
        if paired:
            patch_copy().wait_recv()
        for slot in range(owners):
            total = jnp.zeros(loww.shape[2:], F32)
            for source in range(n):

                @pl.when(z != source)
                def _(slot=slot, source=source):
                    low_arrived(slot, source).wait_recv()

                total = total + loww[slot, source].astype(F32)
            total = total.astype(BF16)
            for step in range(steps):
                lows[slot * steps + step] = total[step * channels : (step + 1) * channels]

    def expand_first(b):
        rows = pl.ds(b * patches, patches)
        values = jnp.dot(tok[rows], embed_ref[...], preferred_element_type=F32)
        inverse = inverse_spread(centered(values))
        for at in range(0, fpad, tile):
            inner = jnp.dot(tok[rows], lows[b, :, at : at + tile], preferred_element_type=F32)
            ubuf[rows, at : at + tile] = gelu(inner * inverse)

    def columns_of(w, members):
        size = shard[w].shape[1] // pieces
        return pl.ds(members[0] * size, len(members) * size)

    def gelu(values):
        return jax.nn.gelu(values, approximate=True).astype(BF16)

    def early_up(members):
        at = columns_of(0, members)
        ubuf[:, at] = gelu(jnp.dot(xbuf[...], up_full[:, at], preferred_element_type=F32))

    def early_down(members):
        at = columns_of(1, members)
        branch = jnp.dot(ubuf[...], down_full[:, at], preferred_element_type=F32)

        def combine(before):
            for b in range(blocks):
                rows = pl.ds(b * patches, patches)
                gate = mod[b, :, pl.ds(wpad + at.start, at.size)]
                here = gate * branch[b * patches : (b + 1) * patches]
                leave[rows, at] = (before(rows) + here).astype(BF16)

        @pl.when(s == 0)
        def _():
            combine(lambda rows: jnp.dot(tok[rows], embed_ref[:, at], preferred_element_type=F32))

        @pl.when(s > 0)
        def _():
            combine(lambda rows: act[rows, at].astype(F32))

        @pl.when(s + 1 < early)
        def _():
            act_copy(0, at, everything).start()

        @pl.when(s + 1 == early)
        def _():
            for i in range(units // 2):
                act_copy(turn(i), at).start()

    streams = works & (s < early)
    begin = min(BEGIN, 2 * count - 1)
    behind = LAG * (last - 1) + 1
    expands = [max(j + behind, begin + 1 + j // 2) for j in range(count)]
    finish = len(runs) + LAG * (last - 1)
    one, rest = streams & (s == 0), streams & (s > 0)
    tasks = [(count + behind, one, prepare_first, None, ())]
    tasks += [(count + behind + b, one, expand_first, None, (b,)) for b in range(blocks)]
    tasks += [(finish, one, early_down, (1, members), (members,)) for members in sets]
    tasks += [(begin, rest, prepare, None, ())]
    tasks += [(t, rest, early_up, (0, members), (members,)) for t, members in zip(expands, sets)]
    tasks += [
        (max(count + j + behind, expands[-1]), rest, early_down, (1, members), (members,))
        for j, members in enumerate(sets)
    ]
    def settle(run, where):
        pl.when(where)(lambda: rest_arrived(*run))

    def do(task):
        _, where, work, run, given = task
        if run is not None:
            settle(run, (s == 0) if where is one else (s > 0))

        @pl.when(where)
        def _():
            if work in (prepare, prepare_first):
                modulations()
            work(*given)

    for w in range(2):
        local_copy(w).wait()

    @pl.when(led & ends)
    def _():
        for at in range(len(runs) - 1):
            waits_early(at)
        release()

    for t in range(finish):
        if t + ahead < len(runs):

            @pl.when(jnp.logical_not(ends))
            def _(t=t):
                send_later(t + ahead)

        for k in range(1, last + 1):
            if 0 <= t - LAG * (k - 1) < len(runs):
                at = t - LAG * (k - 1)
                needs(at, lambda at=at, k=k: relay(runs[at][0], k, runs[at][1]))
        if t == len(runs) - 1:

            @pl.when(led & jnp.logical_not(ends))
            def _():
                release()

        for task in tasks:
            if task[0] == t:
                do(task)
    for task in tasks:
        if task[0] >= finish:
            do(task)

    @pl.when(streams & (s + 1 == early))
    def _():
        for i in range(units // 2, units):
            act_copy(turn(i)).start()

    def drift_copy(slot, d):
        to = {"tm": jnp.where(slot == 0, z, outward) if paired else z, "section": d}
        return pltpu.make_async_remote_copy(
            src_ref=drift_all.at[d, pl.ds(slot * steps, steps)],
            dst_ref=drift,
            send_sem=dr_send.at[slot, d],
            recv_sem=dr_recv,
            device_id=to,
            device_id_type=MESH,
        )

    def project(u):
        rows = pl.ds(pl.multiple_of(u * span, span), span)
        normed = normalize(leave[rows].astype(F32)).astype(BF16)
        fresh = lax.dot_general(
            normed, final_ref[...], (((1,), (1,)), ((), ())), preferred_element_type=F32
        )
        share = sections // cut
        drift_all[pl.ds(lax.rem(u, cut) * share, share), u // cut] = fresh.reshape(
            (share,) + drift_all.shape[2:]
        )

    @pl.when(works & (s >= early))
    def _():
        modulations()

        def one(i, carry):
            u = turn(i)
            b = u // cut
            rows = pl.ds(pl.multiple_of(u * span, span), span)
            act_copy(u).wait_recv()
            x = scaled(b, act[rows].astype(F32))
            before = None
            for at in range(0, fpad, tile):
                inner = jnp.dot(x, up_full[:, at : at + tile], preferred_element_type=F32)
                if before is not None:
                    ubuf[rows, at - tile : at] = gelu(before)
                before = inner
            ubuf[rows, fpad - tile : fpad] = gelu(before)
            branch = jnp.dot(ubuf[rows], down_full[...], preferred_element_type=F32)
            result = (act[rows].astype(F32) + mod[b, :, pl.ds(wpad, wpad)] * branch).astype(BF16)

            project(turn(jnp.maximum(i - 1, 0)))
            leave[rows] = result

            @pl.when(s < sections - 1)
            def _():
                act_copy(u).start()

            if owners > 1:

                @pl.when((s == sections - 1) & (i == steps * cut))
                def _():
                    for d in range(sections):
                        drift_copy(1, d).start()

            return carry

        first_rows = pl.ds(turn(0) * span, span)
        leave[first_rows] = jnp.zeros((span, wpad), BF16)
        lax.fori_loop(0, units, one, 0)

        @pl.when(s == sections - 1)
        def _():
            project(turn(units - 1))
            for d in range(sections - 1):
                drift_copy(0, d).start()

    here = works & (s == sections - 1)

    @pl.when(here)
    def _():
        drift[...] = drift_all[sections - 1, pl.ds(0, steps)]

    @pl.when(jnp.logical_not(here))
    def _():
        drift_copy(0, 0).wait_recv()

    running = jnp.zeros(tot.shape, F32)
    for b in range(steps):
        running = running + steps_ref[b] * drift[b]
    tot[...] = running

    def tot_copy(k):
        return remote(tot, tots.at[k - 1], tot_send.at[k - 1], tot_recv.at[k - 1], "tm", z + k)

    for k in range(1, n):

        @pl.when(z < n - k)
        def _(k=k):
            tot_copy(k).start()

    @pl.when(z == 0)
    def _():
        first[...] = own(0)[...]

    @pl.when(z > 0)
    def _():
        first_copy(1).wait_recv()

    tot_start = first[...]
    new_ref[0] = jnp.zeros(tot.shape, F32)
    for k in range(n - 1, 0, -1):

        @pl.when(z >= k)
        def _(k=k):
            tot_copy(k).wait_recv()
            new_ref[0] = new_ref[0] + tots[k - 1]

    base = tot_start + new_ref[0]
    running = jnp.zeros(tot.shape, F32)
    errors = []
    for b in range(steps):
        fresh = base + running
        running = running + steps_ref[b] * drift[b]
        new_ref[b] = fresh
        delta = jnp.max(jnp.abs(fresh - own(b)[...]), axis=0, keepdims=True)
        errors.append(jnp.broadcast_to(jnp.max(delta, axis=1, keepdims=True), (1, 128)))
    for b in range(steps):
        err_own[pl.ds(b, 1), :] = errors[b]
    for b in range(steps):
        out_ref[b] = jnp.concatenate(
            [new_ref[b, pl.ds(j, out_ref.shape[1], stride=lanes), :] for j in range(lanes)], axis=1
        )
    for b in range(steps, err_own.shape[0]):
        err_own[pl.ds(b, 1), :] = jnp.zeros((1, 128), F32)

    def err_copy(k):
        return remote(
            err_own, errs.at[k - 1], err_send.at[k - 1], err_recv.at[k - 1], "section", lax.rem(s + k, sections)
        )

    for k in range(1, sections):
        err_copy(k).start()
    worst = err_own[...]
    for k in range(1, sections):
        err_copy(k).wait()
        worst = jnp.maximum(worst, errs[k - 1])
    err_ref[...] = worst

    @pl.when(z == 0)
    def _():
        for k in range(1, n):
            first_copy(k).wait_send()

    @pl.when(jnp.logical_not(led & ends))
    def _():
        for at in range(len(runs) - 1):
            needs(at, lambda at=at: own_sends(*runs[at], wait_send))

    @pl.when(led & ends & (s == 0))
    def _():
        for at in range(count + early_waits, len(runs) - 1):
            own_sends(*runs[at], wait_send)

    own_sends(*runs[-1], wait_send)
    for w in range(2):
        for k in range(1, last + 1):
            for case in range(groups):

                @pl.when((g == case) if w else (g == case) & (s > 0))
                def _(w=w, k=k, case=case):
                    for p in range(pieces):
                        if owner_of(w, p) == case:
                            for direction in range(2):

                                @pl.when(has_origin(direction, k))
                                def _(direction=direction, p=p):
                                    @pl.when(has_next(direction))
                                    def _():
                                        along(w, direction, k, p).wait_send()

                                    for j in range(1, groups):
                                        if paired and k == 1:

                                            @pl.when(jnp.logical_not(beside_end(direction)))
                                            def _(j=j):
                                                across(w, direction, k, p, j).wait_send()

                                        else:
                                            across(w, direction, k, p, j).wait_send()

    for owner in range(n):

        @pl.when(z != worker_of(owner, n))
        def _(owner=owner):
            mod_copy(owner).wait_send()

            @pl.when(s == 0)
            def _():
                low_copy(owner).wait_send()

    if paired:

        @pl.when(jnp.logical_not(works) & (s == 0))
        def _():
            patch_copy().wait_send()

    @pl.when(works & (s < sections - 1))
    def _():
        @pl.when(s + 1 < early)
        def _():
            act_copy(0, rows=everything).wait_send()

        @pl.when(s + 1 >= early)
        def _():
            for u in range(units):
                act_copy(u).wait_send()

    @pl.when(here)
    def _():
        for slot in range(owners):
            for d in range(sections if slot else sections - 1):
                drift_copy(slot, d).wait_send()

    for k in range(1, n):

        @pl.when(z < n - k)
        def _(k=k):
            tot_copy(k).wait_send()


def shards(
    sizes,
    states,
    timesteps,
    step_sizes,
    labels,
    class_table,
    embed_weight,
    ada_weight,
    up_weight,
    down_weight,
    final_weight,
):
    n, groups, sections = sizes
    steps, batch, p_size = states.shape
    channels, width = embed_weight.shape
    wide = up_weight.shape[2]
    patches = p_size // channels
    own_patches = patches // sections
    block = round_up(width // n, 16)
    wide_block = round_up(wide // n, 16)
    wpad, fpad = n * block, n * wide_block
    pad = 16
    owners = 2 if n % 4 == 0 else 1
    blocks = owners * steps
    units = blocks * (2 if sections % 2 == 0 else 1)

    cond = condition_rows(timesteps, labels, class_table).reshape(steps, n, width // n)
    cond = jnp.pad(cond.transpose(1, 0, 2), ((0, 0), (0, pad - steps), (0, 0)))
    tokens = states.reshape(steps, p_size // 128, 128)
    embed = pad_blocks(embed_weight, 1, n, block)
    final = pad_blocks(final_weight.T, 1, n, block)
    ada = pad_blocks(ada_weight[0], 1, 2 * n, block)
    up = pad_blocks(pad_blocks(up_weight[0], 1, n, wide_block), 0, 1, block)
    down = pad_blocks(pad_blocks(down_weight[0], 1, n, block), 0, 1, wide_block)
    limit = max(1, 36 // n)
    pieces = max(
        d for d in range(1, limit + 1) if (wpad // 128) % d == 0 and (fpad // 128) % d == 0
    )
    vmem = pltpu.VMEM
    dma = pltpu.SemaphoreType.DMA
    part_shape = (steps, own_patches, channels)
    new_states, errors = pl.pallas_call(
        functools.partial(kernel, (n, groups, sections, width)),
        out_shape=(
            jax.ShapeDtypeStruct((steps, own_patches * channels // 128, 128), F32),
            jax.ShapeDtypeStruct((8, 128), F32),
        ),
        in_specs=[pl.BlockSpec(memory_space=pltpu.SMEM)] + [pl.BlockSpec(memory_space=vmem)] * 7,
        out_specs=(pl.BlockSpec(memory_space=vmem), pl.BlockSpec(memory_space=vmem)),
        scratch_shapes=[
            vmem((wpad, fpad), BF16),
            vmem((fpad, wpad), BF16),
            vmem((n, pad, width // n), BF16),
            vmem((n, steps, 2 * wpad), F32),
            vmem((n * steps, wpad), F32),
            vmem((n, n * steps, block), F32),
            vmem((n, n * steps, block), F32),
            vmem((channels, block), F32),
            vmem((n * steps * channels, block), BF16),
            vmem((n, steps * channels, fpad), BF16),
            vmem((owners, n, steps * channels, fpad), BF16),
            vmem((blocks, channels, fpad), BF16),
            vmem((owners, n, steps, 2 * wpad), F32),
            vmem(part_shape[1:], F32),
            vmem((patches, wpad), F32),
            vmem((blocks * patches, wpad), BF16),
            vmem((blocks * patches, fpad), BF16),
            vmem((blocks, 1, 2 * wpad), F32),
            vmem((blocks * patches, channels), BF16),
            vmem((blocks * patches, wpad), BF16),
            vmem((blocks * patches, wpad), BF16),
            vmem((sections, blocks, own_patches, channels), F32),
            vmem(part_shape, F32),
            vmem(part_shape[1:], F32),
            vmem((max(n - 1, 1),) + part_shape[1:], F32),
            vmem((max(sections - 1, 1), 8, 128), F32),
            vmem((8, 128), F32),
            dma((2, n, pieces)),
            dma((2, 2, n, pieces)),
            dma((2, 2, n, pieces, max(groups - 1, 1))),
            dma((2,)),
            dma((n,)),
            dma((n,)),
            dma((n,)),
            dma((owners, n)),
            dma(()),
            dma(()),
            dma((n,)),
            dma(()),
            dma((units,)),
            dma((units,)),
            dma((owners, sections)),
            dma(()),
            dma((n,)),
            dma((n,)),
            dma((sections,)),
            dma((sections,)),
            pltpu.SemaphoreType.REGULAR,
            dma((n,)),
            dma((n,)),
            dma((n,)),
            dma((owners, n)),
            vmem(part_shape, F32),
            vmem((steps, patches, channels), F32),
        ],
        compiler_params=pltpu.CompilerParams(
            collective_id=0, has_side_effects=True, vmem_limit_bytes=60 * 1024 * 1024
        ),
    )(step_sizes, cond, tokens, embed, final, ada, up, down)
    return new_states.reshape(steps, batch, p_size // sections), errors[:steps, 0]


def solution(mesh):
    sizes = (mesh.shape["tm"], mesh.shape["groups"], mesh.shape["section"])
    return jax.shard_map(
        functools.partial(shards, sizes),
        mesh=mesh,
        in_specs=(
            P(("groups", "tm"), None, None),
            P(("groups", "tm")),
            P(("groups", "tm")),
            P("groups"),
            P(),
            P(),
            P("section", "tm", None),
            P("section", "tm", None),
            P("section", "tm", None),
            P(),
        ),
        out_specs=(P(("groups", "tm"), None, "section"), P(("groups", "tm"))),
        check_vma=False,
    )
```
